32 devices in a mesh: blk: 16 (over z, x, core), rep: 2 (over y).
Axes of the slice: x: 2, y: 2, z: 4, core: 2. Of those that a mesh axis runs over, the one named last changes fastest.
Arguments:
- particles: bfloat16 [896, 2048], P(('blk', 'rep')), may hold values from -0.0029907227 to 0.0029907227
- scores: bfloat16 [896, 2048], P(('blk', 'rep')), may hold values from -60 to 60, as said below
- spread: float32 [1], replicated, may hold values from 0.00034816 to 0.00069632
Outputs:
- direction: float32 [896, 2048], P(('blk', 'rep'))
The draws below stay inside these ranges and needn't reach their ends.
Inputs may be any that keep to these rules, and one draw needn't show every extreme that they name: `scores`: scores of the particles' log posterior.
All inputs are finite; a program needn't handle non-finite values.
Results may differ from the reference program's by a relative error of at most 0.0003.
Values may be sent and summed in bfloat16 or wider, within the bound.
A program may use at most 128 MiB of HBM per device.

```python
import math
import jax
import jax.numpy as jnp
from jax import lax

D = 2048
P_SIZE = 896


def draw_scores(key, part):
    key_common = jax.random.fold_in(key, 11)
    key_rows = jax.random.fold_in(key, 12)
    key_noise = jax.random.fold_in(key, 13)
    upper = 4.0
    common = jax.random.normal(key_common, (D,), jnp.float32)
    row_scale = jnp.exp(jax.random.uniform(key_rows, (P_SIZE, 1), jnp.float32, 0.0, math.log(upper)))
    noise = jax.random.normal(key_noise, (P_SIZE, D), jnp.float32)
    values = jnp.clip(common[None, :] + row_scale * noise, -60.0, 60.0)
    return values.astype(jnp.bfloat16)


def shard_levels(key, dims, cuts, least, largest):
    loudness, own = 1.0, jax.random.fold_in(key, 6)
    for axis_at, blocks in cuts:
        draws = jnp.exp(jax.random.uniform(jax.random.fold_in(own, axis_at), (blocks,), jnp.float32, least / len(cuts), largest / len(cuts)))
        loudness = loudness * jnp.repeat(draws, dims[axis_at] // blocks).reshape([-1 if axis == axis_at else 1 for axis in range(len(dims))])
    return loudness


def gaussian(rng, extent, deviation, reach, split=(), kind=jnp.bfloat16):
    values = deviation * jax.random.normal(rng, extent, jnp.float32)
    if split:
        values = values * shard_levels(rng, extent, split, -0.22, 0.18)
    return jnp.clip(values, -reach, reach).astype(kind)


def setup_inputs(seed: int = 0) -> dict:
    streams_of = jax.random.split(jax.random.key(seed), 4)
    return {
        "particles": gaussian(streams_of[0], (P_SIZE, D), 0.0005, 0.0029907227, ((0, 32),)),
        "scores": draw_scores(jax.random.fold_in(streams_of[3], 71), 0),
        "spread": jnp.clip(jnp.exp(jax.random.uniform(streams_of[2], (1,), jnp.float32, math.log(0.00034816), math.log(0.00069632))), 0.00034816, 0.00069632),
    }


def reference(particles, scores, spread):
    inverse = 1.0 / spread[0]
    population = particles.shape[0]
    particles_wide = particles.astype(jnp.float32)
    norm_all = jnp.sum(particles_wide * particles_wide, axis=1)
    block_rows = math.gcd(population, 512)

    def one_block(block_index):
        first_row = (block_index * block_rows).astype(jnp.int32)
        block_x = lax.dynamic_slice_in_dim(particles, first_row, block_rows, 0)
        block_wide = block_x.astype(jnp.float32)
        block_norm = jnp.sum(block_wide * block_wide, axis=1)
        cross_dots = lax.dot_general(block_x, particles, (((1,), (1,)), ((), ())), preferred_element_type=jnp.float32)
        squared = jnp.maximum(block_norm[:, None] + norm_all[None, :] - 2.0 * cross_dots, 0.0)
        weights = jnp.exp(-squared * inverse)
        weights_low = weights.astype(jnp.bfloat16)
        drive_sum = jnp.dot(weights_low, scores, preferred_element_type=jnp.float32)
        pull_sum = jnp.dot(weights_low, particles, preferred_element_type=jnp.float32)
        row_total = jnp.sum(weights, axis=1)
        return (drive_sum + (2.0 * inverse) * (block_wide * row_total[:, None] - pull_sum)) / population

    blocks = lax.map(one_block, jnp.arange(population // block_rows, dtype=jnp.int32))
    return blocks.reshape(population, particles.shape[1])
```

```python
import functools

import jax
import jax.numpy as jnp
from jax import lax
from jax.experimental import pallas as pl
from jax.experimental.pallas import tpu as pltpu
from jax.sharding import PartitionSpec as P

MESH = pl.DeviceIdType.MESH
GROUP = 4


def kernel(
    n, x_hbm, s_hbm, spread_ref, out_ref, xbuf, sbuf, xpad, spad, pmine, precv, fsend, frecv,
    load_sem, ring_send, ring_recv, chip_send, chip_recv, pair_send, pair_recv,
):
    rows = x_hbm.shape[0]
    groups, _, per_group, pad_rows, half = xpad.shape
    population = rows * 2 * 2 * n
    bufs, pads = (xbuf, sbuf), (xpad, spad)
    b = lax.axis_index("blk")
    rep = lax.axis_index("rep")
    core = b % 2
    q = b // 2
    odd = q % 2
    r = (q // 2) * (1 - odd) + (n - 1 - q // 2) * odd

    def blk_at(position, which):
        up = position // (n // 2)
        chip = (1 - up) * (2 * position) + up * (2 * (n - 1 - position) + 1)
        return chip * 2 + which

    cw = {"blk": blk_at((r + 1) % n, core)}
    ccw = {"blk": blk_at((r + n - 1) % n, core)}
    sibling = {"blk": q * 2 + 1 - core}
    pair = {"rep": 1 - rep}

    order = [0]
    for s in range(1, n // 2):
        order += [s, n - s]
    order.append(n // 2)
    place = {o: divmod(k, GROUP) for k, o in enumerate(order)}

    def slot(a, g, j, o):
        grp, at = place[o]
        return bufs[a].at[grp, j, g * GROUP + at]

    def sem_at(a, j, o):
        return (a * 2 + j) * n + o

    mine = pl.multiple_of(rep * half, 128)
    other = pl.multiple_of((1 - rep) * half, 128)

    loads = []
    for a, ref in enumerate((x_hbm, s_hbm)):
        for grp in range(groups):
            for j in range(2):
                pads[a][grp, j, :, pad_rows - 16:, :] = jnp.zeros(
                    (per_group, 16, half), pads[a].dtype
                )
        copy = pltpu.make_async_copy(
            ref.at[:, pl.ds(mine, half)], slot(a, 0, 0, 0), load_sem.at[a]
        )
        copy.start()
        loads.append(copy)

    barrier = pltpu.get_barrier_semaphore()
    for peer in (cw, ccw, sibling, pair):
        pl.semaphore_signal(barrier, inc=1, device_id=peer, device_id_type=MESH)
    pl.semaphore_wait(barrier, 4)

    started = []

    def remote(src, dst, send, recv, peer):
        copy = pltpu.make_async_remote_copy(
            src_ref=src, dst_ref=dst, send_sem=send, recv_sem=recv,
            device_id=peer, device_id_type=MESH,
        )
        copy.start()
        started.append(copy)

    def reach(j, way):
        return n // 2 - (1 if (j == 0) == (way < 0) else 0)

    def ring(a, j, o, way):
        to = (o + way) % n
        at = sem_at(a, j, to)
        remote(slot(a, 0, j, o), slot(a, 0, j, to), ring_send.at[at],
               ring_recv.at[at], cw if way > 0 else ccw)

    def chip(a, j, o):
        at = sem_at(a, j, o)
        remote(slot(a, 0, j, o), slot(a, 1, j, o), chip_send.at[at],
               chip_recv.at[at], sibling)

    def landed(dst, sem):
        pltpu.make_async_copy(dst, dst, sem).wait()

    def to_pair(a, ref):
        remote(ref.at[:, pl.ds(other, half)], slot(a, 0, 1, 0),
               pair_send.at[a], pair_recv.at[a], pair)

    def first(a, j):
        ring(a, j, 0, 1)
        ring(a, j, 0, -1)
        chip(a, j, 0)

    def hop(a, s, j):
        for way in (1, -1):
            if s <= reach(j, way):
                o = s if way > 0 else n - s
                landed(slot(a, 0, j, o), ring_recv.at[sem_at(a, j, o)])
                if s < reach(j, way):
                    ring(a, j, o, way)
                chip(a, j, o)

    def from_sibling(a, grp):
        for j in range(2):
            for o in order[grp * GROUP:(grp + 1) * GROUP]:
                landed(slot(a, 1, j, o), chip_recv.at[sem_at(a, j, o)])
            for i in range(per_group):
                pads[a][grp, j, i, :rows] = bufs[a][grp, j, i]

    def block(a, grp, j):
        return pads[a][grp, j].reshape(per_group * pad_rows, half)

    def targets():
        return jnp.concatenate([xpad[0, 0, 0], xpad[0, 1, 0]], axis=0)

    def gram(grp):
        from_sibling(0, grp)
        t = targets()
        t_wide = t.astype(jnp.float32)
        t_norm = jnp.sum(t_wide * t_wide, axis=1, keepdims=True)
        for j in range(2):
            source = block(0, grp, j)
            dots = lax.dot_general(
                t, source, (((1,), (1,)), ((), ())), preferred_element_type=jnp.float32
            )
            folded = jnp.zeros((per_group * pad_rows, 128), jnp.float32)
            for c in range(0, half, 128):
                wide = source[:, c:c + 128].astype(jnp.float32)
                folded = folded + wide * wide
            s_norm = jnp.sum(folded.T, axis=0, keepdims=True)
            part = t_norm + s_norm - 2.0 * dots
            pmine[grp, 0, j] = part[:pad_rows]
            pmine[grp, 1, j] = part[pad_rows:]
        remote(pmine.at[grp], precv.at[grp], pair_send.at[3 + grp],
               pair_recv.at[3 + grp], pair)

    to_pair(0, x_hbm)
    to_pair(1, s_hbm)
    loads[0].wait()
    first(0, 0)
    loads[1].wait()
    first(1, 0)
    landed(slot(0, 0, 1, 0), pair_recv.at[0])
    first(0, 1)
    done = 0
    for s in range(1, n // 2 + 1):
        hop(0, s, 0)
        hop(0, s, 1)
        if s == 1:
            landed(slot(1, 0, 1, 0), pair_recv.at[1])
            first(1, 1)
        have = 1 + 2 * s if s < n // 2 else n
        if s < n // 2:
            while (done + 1) * GROUP <= have:
                gram(done)
                done += 1
    hop(1, 1, 0)
    hop(1, 1, 1)
    while done < groups:
        gram(done)
        done += 1

    inverse = 1.0 / jnp.full((1, 1), spread_ref[0], jnp.float32)
    lane = lax.broadcasted_iota(jnp.int32, (1, per_group * pad_rows), 1)
    real = (lane % pad_rows) < rows

    def weights(grp, j, jr):
        total = pmine[grp, jr, j] + precv[grp, 1 - jr, 1 - j]
        return jnp.exp(-jnp.maximum(total, 0.0) * inverse)

    hop(1, 2, 0)
    hop(1, 2, 1)
    row_total = jnp.zeros((2 * pad_rows, 1), jnp.float32)
    pull = jnp.zeros((2 * pad_rows, half), jnp.float32)
    kern = []
    for grp in range(groups):
        landed(precv.at[grp], pair_recv.at[3 + grp])
        for j in range(2):
            w = jnp.concatenate([weights(grp, j, 0), weights(grp, j, 1)], axis=0)
            row_total = row_total + jnp.sum(
                jnp.where(real, w, 0.0), axis=1, keepdims=True
            )
            low = w.astype(jnp.bfloat16)
            kern.append(low)
            pull = pull + jnp.dot(
                low, block(0, grp, j), preferred_element_type=jnp.float32
            )
    base = 2.0 * inverse * (targets().astype(jnp.float32) * row_total - pull)

    done = 0
    for s in range(3, n // 2 + 1):
        hop(1, s, 0)
        hop(1, s, 1)
        have = 1 + 2 * s if s < n // 2 else n
        if s < n // 2:
            while (done + 1) * GROUP <= have:
                from_sibling(1, done)
                for j in range(2):
                    base = base + jnp.dot(
                        kern[2 * done + j], block(1, done, j),
                        preferred_element_type=jnp.float32,
                    )
                done += 1
    for grp in range(done, groups):
        from_sibling(1, grp)

    def finish(jr):
        value = base[jr * pad_rows:(jr + 1) * pad_rows]
        for grp in range(done, groups):
            for j in range(2):
                value = value + jnp.dot(
                    kern[2 * grp + j][jr * pad_rows:(jr + 1) * pad_rows],
                    block(1, grp, j), preferred_element_type=jnp.float32,
                )
        return value / population

    fsend[...] = finish(1)
    remote(fsend, frecv, pair_send.at[2], pair_recv.at[2], pair)
    out_ref[:, pl.ds(mine, half)] = finish(0)[:rows]
    landed(frecv, pair_recv.at[2])
    out_ref[:, pl.ds(other, half)] = frecv[:rows]
    for copy in started:
        copy.wait_send()


def shards(n, particles, scores, spread):
    rows, width = particles.shape
    half = width // 2
    pad_rows = -(-rows // 16) * 16
    groups = n // GROUP
    store = (groups, 2, 2 * GROUP, rows, half)
    padded = (groups, 2, 2 * GROUP, pad_rows, half)
    sums = (groups, 2, 2, pad_rows, 2 * GROUP * pad_rows)
    count = 4 * n
    return pl.pallas_call(
        functools.partial(kernel, n),
        out_shape=jax.ShapeDtypeStruct((rows, width), jnp.float32),
        in_specs=[
            pl.BlockSpec(memory_space=pl.ANY),
            pl.BlockSpec(memory_space=pl.ANY),
            pl.BlockSpec(memory_space=pltpu.SMEM),
        ],
        out_specs=pl.BlockSpec(memory_space=pltpu.VMEM),
        scratch_shapes=[
            pltpu.VMEM(store, particles.dtype),
            pltpu.VMEM(store, scores.dtype),
            pltpu.VMEM(padded, particles.dtype),
            pltpu.VMEM(padded, scores.dtype),
            pltpu.VMEM(sums, jnp.float32),
            pltpu.VMEM(sums, jnp.float32),
            pltpu.VMEM((pad_rows, half), jnp.float32),
            pltpu.VMEM((pad_rows, half), jnp.float32),
            pltpu.SemaphoreType.DMA((2,)),
            pltpu.SemaphoreType.DMA((count,)),
            pltpu.SemaphoreType.DMA((count,)),
            pltpu.SemaphoreType.DMA((count,)),
            pltpu.SemaphoreType.DMA((count,)),
            pltpu.SemaphoreType.DMA((3 + groups,)),
            pltpu.SemaphoreType.DMA((3 + groups,)),
        ],
        compiler_params=pltpu.CompilerParams(
            collective_id=0, has_side_effects=True, vmem_limit_bytes=60 * 2**20
        ),
        name="svgd",
    )(particles, scores, spread)


def kernel_weights(targets, target_norm, source_x, inverse):
    cross_dots = lax.dot_general(
        targets, source_x, (((1,), (1,)), ((), ())), preferred_element_type=jnp.float32
    )
    source_wide = source_x.astype(jnp.float32)
    source_norm = jnp.sum(source_wide * source_wide, axis=1)
    squared = jnp.maximum(target_norm[:, None] + source_norm[None, :] - 2.0 * cross_dots, 0.0)
    return jnp.exp(-squared * inverse)


def plain(particles, scores, spread):
    inverse = 1.0 / spread[0]
    own_count = particles.shape[0]
    population = own_count * lax.axis_size("blk") * lax.axis_size("rep")
    targets = lax.all_gather(particles, "rep", axis=0, tiled=True)
    target_wide = targets.astype(jnp.float32)
    target_norm = jnp.sum(target_wide * target_wide, axis=1)
    stacked = jnp.stack([scores, particles], axis=0)
    source = lax.all_gather(stacked, "blk", axis=1, tiled=True)
    weights = kernel_weights(targets, target_norm, source[1], inverse)
    weights_low = weights.astype(jnp.bfloat16)
    combined_step = jnp.einsum(
        "ij,cjd->cid", weights_low, source, preferred_element_type=jnp.float32
    )
    row_total = jnp.sum(weights, axis=1)
    drive_sum = combined_step[0]
    pull_sum = combined_step[1]
    partial_value = (
        drive_sum + 2.0 * inverse * (target_wide * row_total[:, None] - pull_sum)
    ) / population
    return lax.psum_scatter(partial_value, "rep", scatter_dimension=0, tiled=True)


def solution(mesh):
    n = mesh.shape["blk"] // 2
    even = mesh.shape["rep"] == 2 and mesh.shape["blk"] % 2 == 0 and n % GROUP == 0

    def body(particles, scores, spread):
        need = 24 * mesh.shape["blk"] * particles.size
        if even and n >= 8 and need <= 48 * 2**20:
            return shards(n, particles, scores, spread)
        return plain(particles, scores, spread)

    return jax.shard_map(
        body,
        mesh=mesh,
        in_specs=(P(("blk", "rep"), None), P(("blk", "rep"), None), P()),
        out_specs=P(("blk", "rep"), None),
        check_vma=False,
    )
```
